32 devices in a mesh: dp: 1 (over z), tp: 4 (over y), sp: 8 (over x, core).
Axes of the slice: x: 4, y: 4, z: 1, core: 2. Of those that a mesh axis runs over, the one named last changes fastest.
The devices are a block of a 4x4x8 slice.
Arguments:
- hidden: bfloat16 [32768, 2048], P(('dp', 'sp'))
- w_query: bfloat16 [2048, 2048], P(None, 'tp')
- w_key: bfloat16 [2048, 2048], P(None, 'tp')
- w_value: bfloat16 [2048, 2048], P(None, 'tp')
- w_out: bfloat16 [2048, 2048], P('tp')
- branch_bias: float32 [4, 8], replicated
Outputs:
- output: bfloat16 [32768, 2048], P(('dp', 'sp'), 'tp')
All inputs are finite; a program needn't handle non-finite values.
Results may differ from the reference program's by a relative error of at most 0.00338052.
Values are sent between devices in bfloat16 or wider.
A program may use at most 768 MiB of HBM per device.

```python
import jax
import jax.numpy as jnp
from jax import lax

MODEL_DIM = 2048
NUM_HEADS = 8
NUM_BRANCHES = 4
SEQ_LEN = 32768
SEG_BASE = 2048

HEAD_DIM = MODEL_DIM // NUM_HEADS
LOGIT_SCALE = HEAD_DIM ** -0.5


def setup_inputs(seed: int = 0, part: int = 0) -> dict:
    root_key = jax.random.key(seed)
    hidden_key = jax.random.fold_in(jax.random.fold_in(root_key, 1), part)
    key_list = jax.random.split(jax.random.fold_in(root_key, 2), 5)
    fan_scale = MODEL_DIM ** -0.5

    def weight(key_w, gain_factor):
        drawn = jax.random.normal(key_w, (MODEL_DIM, MODEL_DIM), jnp.float32)
        return (drawn * (gain_factor * fan_scale)).astype(jnp.bfloat16)

    hidden = jax.random.normal(hidden_key, (SEQ_LEN, MODEL_DIM), jnp.float32)
    branch_bias = jax.random.normal(key_list[4], (NUM_BRANCHES, NUM_HEADS), jnp.float32)
    return {'hidden': hidden.astype(jnp.bfloat16), 'w_query': weight(key_list[0], 1.5), 'w_key': weight(key_list[1], 1.5), 'w_value': weight(key_list[2], 1.0), 'w_out': weight(key_list[3], 2.0), 'branch_bias': branch_bias}


def attend_block(blocks):
    q_blk, k_blk, v_blk = blocks
    logits = jnp.dot(q_blk, k_blk.T, preferred_element_type=jnp.float32) * LOGIT_SCALE
    row_max = jnp.max(logits, axis=-1, keepdims=True)
    weights = jnp.exp(logits - row_max)
    row_sum = jnp.sum(weights, axis=-1, keepdims=True)
    numer_sum = jnp.dot(weights.astype(jnp.bfloat16), v_blk, preferred_element_type=jnp.float32)
    return numer_sum / row_sum, (row_max + jnp.log(row_sum))[:, 0]


def branch_attention(q_all, k_all, v_all, branch):
    dil_rate = 2 ** branch
    num_segs = SEQ_LEN // (SEG_BASE * dil_rate)
    phase_ok = jnp.arange(NUM_HEADS)[:, None] % dil_rate == jnp.arange(dil_rate)[None, :]
    phase_f = phase_ok.astype(jnp.float32)

    def pick_rows(source):
        split_rows = source.astype(jnp.float32).reshape(num_segs, SEG_BASE, dil_rate, NUM_HEADS, HEAD_DIM)
        chosen = jnp.einsum('asihd,hi->ahsd', split_rows, phase_f).astype(jnp.bfloat16)
        return chosen.reshape(num_segs * NUM_HEADS, SEG_BASE, HEAD_DIM)

    attn_out, log_norm = lax.map(attend_block, (pick_rows(q_all), pick_rows(k_all), pick_rows(v_all)))
    attn_out = attn_out.reshape(num_segs, NUM_HEADS, SEG_BASE, HEAD_DIM)
    log_norm = log_norm.reshape(num_segs, NUM_HEADS, SEG_BASE)
    out_full = jnp.einsum('ahsd,hi->asihd', attn_out, phase_f).reshape(SEQ_LEN, NUM_HEADS, HEAD_DIM)
    lse_full = jnp.einsum('ahs,hi->asih', log_norm, phase_f).reshape(SEQ_LEN, NUM_HEADS)
    mask_full = jnp.broadcast_to(phase_ok.T[None, None], (num_segs, SEG_BASE, dil_rate, NUM_HEADS)).reshape(SEQ_LEN, NUM_HEADS)
    return out_full, lse_full, mask_full


def reference(hidden, w_query, w_key, w_value, w_out, branch_bias):
    def project(weight):
        return jnp.dot(hidden, weight, preferred_element_type=jnp.float32).astype(jnp.bfloat16).reshape(SEQ_LEN, NUM_HEADS, HEAD_DIM)

    q_all = project(w_query)
    k_all = project(w_key)
    v_all = project(w_value)
    for branch in range(NUM_BRANCHES):
        out_full, lse_full, mask_full = branch_attention(q_all, k_all, v_all, branch)
        branch_score = jnp.where(mask_full, lse_full + branch_bias[branch][None, :], -jnp.inf)
        if branch == 0:
            run_num = out_full
            run_max = branch_score
            run_den = jnp.ones_like(branch_score)
        else:
            new_max = jnp.maximum(run_max, branch_score)
            keep_old = jnp.exp(run_max - new_max)
            take_new = jnp.exp(branch_score - new_max)
            run_num = run_num * keep_old[..., None] + out_full * take_new[..., None]
            run_den = run_den * keep_old + take_new
            run_max = new_max
    combined = (run_num / run_den[..., None]).astype(jnp.bfloat16).reshape(SEQ_LEN, MODEL_DIM)
    return jnp.dot(combined, w_out, preferred_element_type=jnp.float32).astype(jnp.bfloat16)
```

```python
import functools

import jax
import jax.numpy as jnp
from jax import lax
from jax.experimental import pallas as pl
from jax.experimental.pallas import tpu as pltpu
from jax.sharding import PartitionSpec as P

SEG_BASE = 2048
PHASES = 8
SLOT = (0, 4, 2, 6, 1, 5, 3, 7)
F32 = jnp.float32
BF16 = jnp.bfloat16


def _layer(dims, hidden, wq, wk, wv, wo, bias, out, hbuf, wqkv, pf, qs, ks, vs, k2, v2, k3, v3, wfull, osend, ofull,
           relay, outsend, orelay, h_sem, w_sem, wo_loc, wo_s, wo_r, wof_s, wof_r, wod_s, wod_r, kv2_s, kv2_r, kv3_s,
           kv3_r, o_s, o_r, r_s, r_r, f_s, f_r, u_s, u_r, ur_s, ur_r, uf_s, uf_r, u_loc):
    block_rows, half, dim, scale = dims
    tp_size = 4
    y = lax.axis_index('tp')
    sp = lax.axis_index('sp')
    core = lax.rem(sp, 2)
    up = lax.rem(y + 1, tp_size)
    far = lax.rem(y + 2, tp_size)
    down = lax.rem(y + 3, tp_size)
    tokens = hidden.shape[0]
    num_blocks = tokens // block_rows
    phase_rows = block_rows // PHASES
    quarter = dim // 2
    cols = outsend.shape[-1]

    def sp_peer(dist):
        base = (sp // 4) * 4
        pos = lax.rem(sp, 4)
        if dist == 1:
            other = pos + 1 - 2 * lax.rem(pos, 2)
        elif dist == 2:
            other = lax.rem(pos + 2, 4)
        else:
            other = 3 - pos
        return base + other

    partner = sp_peer(1)

    def remote(src, dst, ssem, rsem, dev):
        return pltpu.make_async_remote_copy(src_ref=src, dst_ref=dst, send_sem=ssem, recv_sem=rsem, device_id=dev,
                                            device_id_type=pl.DeviceIdType.MESH)

    def load_hidden(b):
        slot = lax.rem(b, 3)
        return pltpu.make_async_copy(hidden.at[pl.ds(b * block_rows, block_rows), :], hbuf.at[slot], h_sem.at[slot])

    w_loads = [pltpu.make_async_copy(w, wqkv.at[n], w_sem.at[n]) for n, w in enumerate((wq, wk, wv))]
    load_hidden(0).start()
    w_loads[0].start()
    load_hidden(1).start()
    w_loads[1].start()
    w_loads[2].start()
    wo_local = [pltpu.make_async_copy(wo.at[pl.ds(i * dim, dim), :], wfull.at[y, i], wo_loc.at[i]) for i in range(2)]
    for c in wo_local:
        c.start()

    barrier = pltpu.get_barrier_semaphore()
    peers = [{'tp': up}, {'tp': far}, {'tp': down}] + [{'sp': sp_peer(d)} for d in (1, 2, 3)]
    for dev in peers:
        pl.semaphore_signal(barrier, inc=1, device_id=dev, device_id_type=pl.DeviceIdType.MESH)
    pl.semaphore_wait(barrier, len(peers))

    dirs = (up, down)
    wo_send = [remote(wo.at[pl.ds(core * dim, dim), :], wfull.at[y, core], wo_s.at[n], wo_r.at[n], {'tp': dirs[n]})
               for n in range(2)]
    for c in wo_send:
        c.start()
    near = (down, up)
    wo_part = [pl.ds(0, quarter), pl.ds(quarter, quarter)]
    wo_fwd = [remote(wfull.at[near[n], core, wo_part[n]], wfull.at[near[n], core, wo_part[n]], wof_s.at[n],
                     wof_r.at[n], {'tp': dirs[n]}) for n in range(2)]
    wo_d2d = [remote(wfull.at[near[n], core], wfull.at[near[n], core], wod_s.at[n], wod_r.at[n], {'sp': partner})
              for n in range(2)]
    wo_d2d += [remote(wfull.at[far, core, wo_part[n]], wfull.at[far, core, wo_part[n]], wod_s.at[2 + n],
                      wod_r.at[2 + n], {'sp': partner}) for n in range(2)]

    w_loads[0].wait()
    w_loads[1].wait()
    w_loads[2].wait()

    def project(b, carry):
        load_hidden(b).wait()

        @pl.when(b + 2 < num_blocks)
        def _():
            load_hidden(b + 2).start()

        rows = hbuf[lax.rem(b, 3)]
        s = b // (num_blocks // 2)
        r0 = pl.multiple_of(lax.rem(b, num_blocks // 2) * phase_rows, phase_rows)
        for n, dst in enumerate((qs, ks, vs)):
            for i in range(2):
                res = jnp.dot(rows, wqkv[n, :, i * dim:(i + 1) * dim], preferred_element_type=F32)
                if n == 0:
                    res = res * scale
                for c in range(dim // 128):
                    buf = pf.at[n * 2 + i, c]
                    buf[...] = res[:, c * 128:(c + 1) * 128]
                    for ph in range(PHASES):
                        picked = buf[pl.ds(ph, phase_rows, stride=PHASES), :]
                        dst[i, SLOT[ph], s, pl.ds(r0, phase_rows), c * 128:(c + 1) * 128] = picked.astype(BF16)
        return carry

    lax.fori_loop(0, num_blocks, project, 0)

    u_y = lax.rem(y, 2) * 2 + y // 2
    pair_y = lax.rem(y, 2) * 2
    kv2 = []
    kv3 = []
    for n, (src, two, three) in enumerate(((ks, k2, k3), (vs, v2, v3))):
        for i in range(2):
            kv2.append(remote(src.at[i, pl.ds(4 * i + pair_y, 2)], two.at[i], kv2_s.at[n, i], kv2_r.at[n, i],
                              {'sp': partner}))
            for d in (2, 3, 1):
                kv3.append(remote(src.at[i, 4 * i + u_y], three.at[d - 1, i], kv3_s.at[d - 1, n, i],
                                  kv3_r.at[d - 1, n, i], {'sp': sp_peer(d)}))
    for c in kv2:
        c.start()
    for c in kv3:
        c.start()
    for n in range(2):
        wo_send[n].wait_recv()
        wo_fwd[n].start()
    for n in range(2):
        wo_d2d[n].start()

    def attend(q, keys, values):
        logits = [lax.dot_general(q, k, (((1,), (1,)), ((), ())), preferred_element_type=F32) for k in keys]
        top = logits[0]
        for x in logits[1:]:
            top = jnp.maximum(top, x)
        top = jnp.max(top, axis=1, keepdims=True)
        total = None
        numer = None
        for x, v in zip(logits, values):
            e = jnp.exp(x - top)
            total = e if total is None else total + e
            part = jnp.dot(e.astype(BF16), v, preferred_element_type=F32)
            numer = part if numer is None else numer + part
        return numer, top, jnp.sum(total, axis=1, keepdims=True)

    def head_step(t, s, i, level, dst):
        u = lax.rem(t, 2) * 2 + t // 2
        slot_a = 4 * i + u
        slot_b = 4 * (1 - i) + u
        q_a = qs[i, slot_a, s]
        q_b = qs[i, slot_b, s]
        n0, m0, l0 = attend(jnp.concatenate([q_a, q_b], axis=0), [ks[i, c, s] for c in range(PHASES)],
                            [vs[i, c, s] for c in range(PHASES)])
        dst[1 - i] = (n0[half:] / l0[half:]).astype(BF16)
        parts = [(n0[:half], m0[:half], l0[:half])]
        tiles = [(4 * i + c, h) for c in range(4) for h in range(2)]
        parts.append(attend(q_a, [ks[i, c, h] for c, h in tiles], [vs[i, c, h] for c, h in tiles]))
        if level >= 1:
            tiles = [(c, h) for c in range(2) for h in range(2)]
            base = 4 * i + pair_y
            parts.append(attend(q_a, [ks[i, base + c, h] for c, h in tiles] + [k2[i, c, h] for c, h in tiles],
                                [vs[i, base + c, h] for c, h in tiles] + [v2[i, c, h] for c, h in tiles]))
        if level >= 2:
            mine = 4 * i + u_y
            tiles = [(d, h) for d in range(3) for h in range(2)]
            parts.append(attend(q_a, [ks[i, mine, h] for h in range(2)] + [k3[d, i, h] for d, h in tiles],
                                [vs[i, mine, h] for h in range(2)] + [v3[d, i, h] for d, h in tiles]))
        scores = [m + bias[j, 2 * y + i] for j, (_, m, _) in enumerate(parts)]
        best = functools.reduce(jnp.maximum, scores)
        num = None
        den = None
        for (n, _, l), sc in zip(parts, scores):
            w = jnp.exp(sc - best)
            num = n * w if num is None else num + n * w
            den = l * w if den is None else den + l * w
        dst[i] = (num / den).astype(BF16)

    def o_direct(n, s, i):
        dev = lax.rem(y + 1 + 2 * n, tp_size)
        return remote(osend.at[n, s, i], ofull.at[y, s, i], o_s.at[n, s, i], o_r.at[n, s, i], {'tp': dev})

    def o_relay(s, i):
        dev = lax.rem(y + 1 + 2 * i, tp_size)
        return remote(osend.at[2, s, i], relay.at[s, i], r_s.at[s, i], r_r.at[s, i], {'tp': dev})

    def o_forward(s, i):
        origin = near[i]
        return remote(relay.at[s, i], ofull.at[origin, s, i], f_s.at[s, i], f_r.at[s, i], {'tp': dirs[i]})

    def forward_relay(s):
        for i in range(2):
            o_relay(s, i).wait_recv()
            o_forward(s, i).start()

    def attention_half(s, carry):
        def near_step(j, c):
            n = j // 2
            i = lax.rem(j, 2)
            head_step(lax.rem(y + 1 + 2 * n, tp_size), s, i, 0, osend.at[n, s, i])
            o_direct(n, s, i).start()
            return c

        lax.fori_loop(0, 4, near_step, 0)

        @pl.when(s == 0)
        def _():
            for c in kv2:
                c.wait_recv()

        @pl.when(s == 1)
        def _():
            forward_relay(0)
            for n in range(2):
                wo_fwd[n].wait_recv()
                wo_d2d[2 + n].start()

        def far_step(i, c):
            head_step(far, s, i, 1, osend.at[2, s, i])
            o_relay(s, i).start()
            return c

        lax.fori_loop(0, 2, far_step, 0)

        @pl.when(s == 0)
        def _():
            for c in kv3:
                c.wait_recv()

        def own_step(i, c):
            head_step(y, s, i, 2, ofull.at[y, s, i])
            return c

        lax.fori_loop(0, 2, own_step, 0)
        return carry

    lax.fori_loop(0, 2, attention_half, 0)
    forward_relay(1)

    for c in wo_local:
        c.wait()
    for c in wo_d2d:
        c.wait_recv()

    def out_rows(src, i, s):
        return out.at[2 * src + i, pl.ds(s * half, half), :]

    def u_direct(n, s, i):
        return remote(outsend.at[s, n, i], out_rows(y, i, s), u_s.at[n, s, i], u_r.at[n, s, i], {'tp': dirs[n]})

    def u_relay(s, i):
        return remote(outsend.at[s, 2, i], orelay.at[s, i], ur_s.at[s, i], ur_r.at[s, i], {'tp': dirs[i]})

    def u_forward(s, i):
        return remote(orelay.at[s, i], out_rows(near[i], i, s), uf_s.at[s, i], uf_r.at[s, i], {'tp': dirs[i]})

    def u_own(s, i):
        return pltpu.make_async_copy(outsend.at[s, 3, i], out_rows(y, i, s), u_loc.at[s, i])

    def out_half(s):
        for i in range(2):
            for n in range(2):
                o_direct(n, s, i).wait_recv()
            o_forward(s, i).wait_recv()
        for n, t in ((2, far), (0, up), (1, down), (3, y)):
            c0 = pl.multiple_of(t * cols, cols)
            acc = None
            for src in range(tp_size):
                for i in range(2):
                    lhs = ofull[src, s, i].reshape(2 * half, dim)
                    part = jnp.dot(lhs, wfull[src, i, :, pl.ds(c0, cols)], preferred_element_type=F32)
                    acc = part if acc is None else acc + part
            outsend[s, n] = acc.astype(BF16).reshape(2, half, cols)
            for i in range(2):
                if n == 2:
                    u_relay(s, i).start()
                elif n == 3:
                    u_own(s, i).start()
                else:
                    u_direct(n, s, i).start()

    def forward_out(s):
        for i in range(2):
            u_relay(s, i).wait_recv()
            u_forward(s, i).start()

    out_half(0)
    forward_out(0)
    out_half(1)
    forward_out(1)

    for c in wo_send + wo_fwd + wo_d2d + kv2 + kv3:
        c.wait_send()
    for s in range(2):
        for i in range(2):
            for n in range(2):
                o_direct(n, s, i).wait_send()
                u_direct(n, s, i).wait()
            o_relay(s, i).wait_send()
            o_forward(s, i).wait_send()
            u_relay(s, i).wait_send()
            u_forward(s, i).wait()
            u_own(s, i).wait()


def _natural_order(src, out, buf):
    rows = src.shape[1]
    for c in range(src.shape[2] // 128):
        lanes = slice(c * 128, (c + 1) * 128)
        for ph in range(PHASES):
            buf[c, pl.ds(ph, rows, stride=PHASES), :] = src[ph, :, lanes].astype(F32)
        out[:, lanes] = buf[c].astype(BF16)


def solution(mesh):
    head_groups = mesh.shape['tp']

    def device_fn(hidden, w_query, w_key, w_value, w_out, branch_bias):
        tokens, model_width = hidden.shape
        num_branches, num_heads = branch_bias.shape
        dim = model_width // num_heads
        local_cols = w_query.shape[1]
        cols = model_width // head_groups
        half = tokens // PHASES // 2
        block_rows = min(256, tokens // 4)
        assert head_groups == 4 and num_branches == 4 and num_heads == PHASES and local_cols == 2 * dim
        assert half * PHASES == seg_rows(tokens)
        any_spec = pl.BlockSpec(memory_space=pl.ANY)
        dma = pltpu.SemaphoreType.DMA
        tile = (half, dim)
        vm = lambda *shape: pltpu.VMEM(shape, BF16)
        phase_major = pl.pallas_call(
            functools.partial(_layer, (block_rows, half, dim, dim ** -0.5)),
            out_shape=jax.ShapeDtypeStruct((PHASES, 2 * half, cols), BF16),
            in_specs=[any_spec] * 5 + [pl.BlockSpec(memory_space=pltpu.SMEM)],
            out_specs=any_spec,
            scratch_shapes=[
                vm(3, block_rows, model_width), vm(3, model_width, local_cols),
                pltpu.VMEM((6, dim // 128, block_rows, 128), F32),
                vm(2, PHASES, 2, *tile), vm(2, PHASES, 2, *tile), vm(2, PHASES, 2, *tile),
                vm(2, 2, 2, *tile), vm(2, 2, 2, *tile), vm(3, 2, 2, *tile), vm(3, 2, 2, *tile),
                vm(4, 2, dim, model_width),
                vm(3, 2, 2, 2, *tile), vm(4, 2, 2, 2, *tile), vm(2, 2, 2, *tile),
                vm(2, 4, 2, half, cols), vm(2, 2, half, cols),
                dma((3,)), dma((3,)), dma((2,)),
                dma((2,)), dma((2,)), dma((2,)), dma((2,)), dma((4,)), dma((4,)),
                dma((2, 2)), dma((2, 2)), dma((3, 2, 2)), dma((3, 2, 2)),
                dma((2, 2, 2)), dma((2, 2, 2)), dma((2, 2)), dma((2, 2)), dma((2, 2)), dma((2, 2)),
                dma((2, 2, 2)), dma((2, 2, 2)), dma((2, 2)), dma((2, 2)), dma((2, 2)), dma((2, 2)), dma((2, 2)),
            ],
            compiler_params=pltpu.CompilerParams(collective_id=0, has_side_effects=True,
                                                 vmem_limit_bytes=67043328),
            name='layer',
        )(hidden, w_query, w_key, w_value, w_out, branch_bias)
        rows = min(64, half)
        return pl.pallas_call(
            _natural_order,
            grid=(2 * half // rows,),
            in_specs=[pl.BlockSpec((PHASES, rows, cols), lambda b: (0, b, 0))],
            out_specs=pl.BlockSpec((PHASES * rows, cols), lambda b: (b, 0)),
            out_shape=jax.ShapeDtypeStruct((tokens, cols), BF16),
            scratch_shapes=[pltpu.VMEM((cols // 128, PHASES * rows, 128), F32)],
            name='natural_order',
        )(phase_major)

    return jax.shard_map(device_fn, mesh=mesh, in_specs=(P(('dp', 'sp'), None), P(None, 'tp'), P(None, 'tp'), P(None, 'tp'), P('tp', None), P(None, None)), out_specs=P(('dp', 'sp'), 'tp'), check_vma=False)


def seg_rows(tokens):
    return SEG_BASE if tokens >= 2 * SEG_BASE else tokens // 2
```

```python
import functools

import jax
import jax.numpy as jnp
from jax import lax
from jax.experimental import pallas as pl
from jax.experimental.pallas import tpu as pltpu
from jax.sharding import PartitionSpec as P

SEG_BASE = 2048
PHASES = 8
SLOT = (0, 4, 2, 6, 1, 5, 3, 7)
F32 = jnp.float32
BF16 = jnp.bfloat16


def _layer(dims, hidden, wq, wk, wv, wo, bias, out, hbuf, wqkv, pf, qs, ks, vs, k2, v2, k3, v3, wfull, osend, ofull,
           relay_a, relay_b, orelay, h_sem, w_sem, wo_loc, wy_s, wy_r, wyf_s, wyf_r, wx_s, wx_r, wxf_s, wxf_r,
           wd_s, wd_r, wdf_s, wdf_r, kv2_s, kv2_r, kv3_s, kv3_r, oa_s, oa_r, ra_s, ra_r, fa_s, fa_r, ob_s, ob_r, rb_s,
           rb_r, fb_s, fb_r, u_s, u_r, ur_s, ur_r, uf_s, uf_r, u_loc):
    block_rows, half, dim, scale = dims
    tp_size = 4
    y = lax.axis_index('tp')
    sp = lax.axis_index('sp')
    up = lax.rem(y + 1, tp_size)
    far = lax.rem(y + 2, tp_size)
    down = lax.rem(y + 3, tp_size)
    tokens = hidden.shape[0]
    num_blocks = tokens // block_rows
    half_blocks = num_blocks // 2
    phase_rows = block_rows // PHASES
    slices, _, piece, _ = wfull.shape
    cols = orelay.shape[-1]

    def sp_peer(dist):
        base = (sp // 4) * 4
        pos = lax.rem(sp, 4)
        if dist == 1:
            other = pos + 1 - 2 * lax.rem(pos, 2)
        elif dist == 2:
            other = lax.rem(pos + 2, 4)
        else:
            other = 3 - pos
        return base + other

    partner = sp_peer(1)
    right = lax.rem(sp + 2, slices)
    opposite = lax.rem(sp + slices // 2, slices)
    left = lax.rem(sp + slices - 2, slices)

    def remote(src, dst, ssem, rsem, dev):
        return pltpu.make_async_remote_copy(src_ref=src, dst_ref=dst, send_sem=ssem, recv_sem=rsem, device_id=dev,
                                            device_id_type=pl.DeviceIdType.MESH)

    def load_hidden(b):
        slot = lax.rem(b, 2)
        return pltpu.make_async_copy(hidden.at[pl.ds(b * block_rows, block_rows), :], hbuf.at[slot], h_sem.at[slot])

    w_loads = [pltpu.make_async_copy(w, wqkv.at[n], w_sem.at[n]) for n, w in enumerate((wq, wk, wv))]
    load_hidden(0).start()
    w_loads[0].start()
    w_loads[1].start()
    w_loads[2].start()
    wo_local = [pltpu.make_async_copy(wo.at[pl.ds(j * piece, piece), :], wfull.at[j, y], wo_loc.at[j])
                for j in range(slices)]
    barrier = pltpu.get_barrier_semaphore()
    peers = [{'tp': up}, {'tp': far}, {'tp': down}, {'sp': partner}, {'sp': right}, {'sp': left}]
    for dev in peers:
        pl.semaphore_signal(barrier, inc=1, device_id=dev, device_id_type=pl.DeviceIdType.MESH)

    dirs = (up, down)
    near = (down, up)
    xdirs = (right, left)
    xnear = (left, right)
    part = [pl.ds(0, piece // 2), pl.ds(piece // 2, piece // 2)]
    wo_y = [remote(wo.at[pl.ds(pl.multiple_of(sp * piece, piece), piece), :], wfull.at[sp, y], wy_s.at[n], wy_r.at[n],
                   {'tp': dirs[n]}) for n in range(2)]
    wo_yf = [remote(wfull.at[sp, near[n], part[n]], wfull.at[sp, near[n], part[n]], wyf_s.at[n], wyf_r.at[n],
                    {'tp': dirs[n]}) for n in range(2)]
    others = (up, far, down)

    def wo_x(n, k):
        ref = wfull.at[sp, others[k]]
        return remote(ref, ref, wx_s.at[n, k], wx_r.at[n, k], {'sp': xdirs[n]})

    def wo_xf(n, k):
        ref = wfull.at[xnear[n], others[k], part[n]]
        return remote(ref, ref, wxf_s.at[n, k], wxf_r.at[n, k], {'sp': xdirs[n]})

    def wo_d(j, k):
        ref = wfull.at[(sp, left, right)[j], others[k]]
        return remote(ref, ref, wd_s.at[j, k], wd_r.at[j, k], {'sp': partner})

    def wo_df(n, k):
        ref = wfull.at[opposite, others[k], part[n]]
        return remote(ref, ref, wdf_s.at[n, k], wdf_r.at[n, k], {'sp': partner})

    u_y = lax.rem(y, 2) * 2 + y // 2
    pair_y = lax.rem(y, 2) * 2
    kv = ((ks, k2, k3), (vs, v2, v3))

    def kv2(n, i):
        src, two, _ = kv[n]
        return remote(src.at[i, pl.ds(4 * i + pair_y, 2)], two.at[i], kv2_s.at[n, i], kv2_r.at[n, i], {'sp': partner})

    def kv3(d, n, i):
        src, _, three = kv[n]
        ref = three.at[1, i] if d == 3 else src.at[i, 4 * i + u_y]
        return remote(ref, three.at[d - 1, i], kv3_s.at[d - 1, n, i], kv3_r.at[d - 1, n, i],
                      {'sp': partner if d == 3 else sp_peer(d)})

    def attend(q, keys, values):
        logits = [lax.dot_general(q, k, (((1,), (1,)), ((), ())), preferred_element_type=F32) for k in keys]
        top = logits[0]
        for x in logits[1:]:
            top = jnp.maximum(top, x)
        top = jnp.max(top, axis=1, keepdims=True)
        total = None
        numer = None
        for x, v in zip(logits, values):
            e = jnp.exp(x - top)
            total = e if total is None else total + e
            piece_sum = jnp.dot(e.astype(BF16), v, preferred_element_type=F32)
            numer = piece_sum if numer is None else numer + piece_sum
        return numer, top, jnp.sum(total, axis=1, keepdims=True)

    def slot_of(t):
        return lax.rem(t, 2) * 2 + t // 2

    def step_b(s, i, t0, t1, dst0, dst1):
        q = jnp.concatenate([qs[i, 4 * (1 - i) + slot_of(t0), s], qs[i, 4 * (1 - i) + slot_of(t1), s]], axis=0)
        n, _, l = attend(q, [ks[i, c, s] for c in range(PHASES)], [vs[i, c, s] for c in range(PHASES)])
        o = (n / l).astype(BF16)
        dst0[...] = o[:half]
        dst1[...] = o[half:]

    def step_a(t, i, level, dst, s=None):
        slot = 4 * i + slot_of(t)
        zero = [attend(qs[i, slot, h], [ks[i, c, h] for c in range(PHASES)], [vs[i, c, h] for c in range(PHASES)])
                for h in (range(2) if s is None else (s,))]
        if s is None:
            parts = [tuple(jnp.concatenate([a, b], axis=0) for a, b in zip(*zero))]
            q = qs[i, slot].reshape(2 * half, dim)
        else:
            parts = zero
            q = qs[i, slot, s]
        tiles = [(4 * i + c, h) for c in range(4) for h in range(2)]
        parts.append(attend(q, [ks[i, c, h] for c, h in tiles], [vs[i, c, h] for c, h in tiles]))
        if level >= 1:
            tiles = [(c, h) for c in range(2) for h in range(2)]
            base = 4 * i + pair_y
            parts.append(attend(q, [ks[i, base + c, h] for c, h in tiles] + [k2[i, c, h] for c, h in tiles],
                                [vs[i, base + c, h] for c, h in tiles] + [v2[i, c, h] for c, h in tiles]))
        if level >= 2:
            mine = 4 * i + u_y
            tiles = [(d, h) for d in range(3) for h in range(2)]
            parts.append(attend(q, [ks[i, mine, h] for h in range(2)] + [k3[d, i, h] for d, h in tiles],
                                [vs[i, mine, h] for h in range(2)] + [v3[d, i, h] for d, h in tiles]))
        scores = [m + bias[j, 2 * y + i] for j, (_, m, _) in enumerate(parts)]
        best = functools.reduce(jnp.maximum, scores)
        num = None
        den = None
        for (n, _, l), sc in zip(parts, scores):
            w = jnp.exp(sc - best)
            num = n * w if num is None else num + n * w
            den = l * w if den is None else den + l * w
        dst[...] = (num / den).astype(BF16).reshape(dst.shape)

    def along(n):
        return {'tp': lax.rem(y + 1 + 2 * n, tp_size)}

    def a_direct(n, i):
        return remote(osend.at[n, i, i], ofull.at[y, i, i], oa_s.at[n, i], oa_r.at[n, i], along(n))

    def a_relay(i):
        return remote(osend.at[2, i, i], relay_a.at[i], ra_s.at[i], ra_r.at[i], along(i))

    def origin(n):
        return lax.rem(y + 3 - 2 * n, tp_size)

    def a_forward(i):
        return remote(relay_a.at[i], ofull.at[origin(i), i, i], fa_s.at[i], fa_r.at[i], along(i))

    def b_direct(n, s, i):
        return remote(osend.at[n, i, 1 - i, s], ofull.at[y, i, 1 - i, s], ob_s.at[n, s, i], ob_r.at[n, s, i], along(n))

    def b_relay(s, i):
        return remote(osend.at[2, i, 1 - i, s], relay_b.at[s, i], rb_s.at[s, i], rb_r.at[s, i], along(i))

    def b_forward(s, i):
        return remote(relay_b.at[s, i], ofull.at[origin(i), i, 1 - i, s], fb_s.at[s, i], fb_r.at[s, i], along(i))

    def forward_b(s):
        for i in range(2):
            b_relay(s, i).wait_recv()
            b_forward(s, i).start()

    for c in w_loads:
        c.wait()

    def first(s, carry):
        def project(r, c):
            b = s * half_blocks + r
            load_hidden(b).wait()

            @pl.when(b + 1 < num_blocks)
            def _():
                load_hidden(b + 1).start()

            @pl.when(b == 1)
            def _():
                pl.semaphore_wait(barrier, len(peers))
                for c in wo_y + wo_local:
                    c.start()

            @pl.when(b == half_blocks - 2)
            def _():
                for n in range(2):
                    wo_y[n].wait_recv()
                    wo_yf[n].start()

            @pl.when(b == half_blocks + 1)
            def _():
                for c in wo_yf:
                    c.wait_recv()
                for k in range(3):
                    for n in range(2):
                        wo_x(n, k).start()
                    wo_d(0, k).start()

            @pl.when(b == num_blocks - 2)
            def _():
                forward_b(0)

            rows = hbuf[lax.rem(b, 2)]
            r0 = pl.multiple_of(r * phase_rows, phase_rows)
            for n, dst in enumerate((qs, ks, vs)):
                for i in range(2):
                    res = jnp.dot(rows, wqkv[n, :, i * dim:(i + 1) * dim], preferred_element_type=F32)
                    if n == 0:
                        res = res * scale
                    for g in range(dim // 128):
                        buf = pf.at[n * 2 + i, g]
                        buf[...] = res[:, g * 128:(g + 1) * 128]
                        for ph in range(PHASES):
                            picked = buf[pl.ds(ph, phase_rows, stride=PHASES), :]
                            dst[i, SLOT[ph], s, pl.ds(r0, phase_rows), g * 128:(g + 1) * 128] = picked.astype(BF16)
            return c

        lax.fori_loop(0, half_blocks, project, 0)

        @pl.when(s == 1)
        def _():
            for i in range(2):
                for n in range(2):
                    kv2(n, i).start()
                    for d in (2, 1):
                        kv3(d, n, i).start()

        def b_pair(i, c):
            step_b(s, i, far, y, osend.at[2, i, 1 - i, s], ofull.at[y, i, 1 - i, s])
            step_b(s, i, up, down, osend.at[0, i, 1 - i, s], osend.at[1, i, 1 - i, s])
            b_relay(s, i).start()
            for n in range(2):
                b_direct(n, s, i).start()
            return c

        lax.fori_loop(0, 2, b_pair, 0)
        return carry

    lax.fori_loop(0, 2, first, 0)

    def outsend(n, i, rows=slice(0, 2 * half)):
        k = 2 * n + i
        per = wqkv.shape[1] // (2 * half)
        return wqkv.at[k // per, pl.ds(pl.multiple_of(lax.rem(k, per) * 2 * half, 2 * half) + rows.start, rows.stop - rows.start), :]

    def u_direct(n, i):
        return remote(outsend(n, i), out.at[2 * y + i], u_s.at[n, i], u_r.at[n, i], {'tp': dirs[n]})

    def u_relay(i, n):
        return remote(outsend(2, i, slice(n * half, (n + 1) * half)), orelay.at[i, n], ur_s.at[i, n], ur_r.at[i, n],
                      {'tp': dirs[n]})

    def u_forward(i, n):
        return remote(orelay.at[i, n], out.at[2 * near[n] + i, pl.ds(n * half, half)], uf_s.at[i, n], uf_r.at[i, n],
                      {'tp': dirs[n]})

    def forward_u(i):
        for n in range(2):
            u_relay(i, n).wait_recv()
            u_forward(i, n).start()

    def u_own(i):
        return pltpu.make_async_copy(outsend(3, i), out.at[2 * y + i], u_loc.at[i])

    for k in range(3):
        for n in range(2):
            wo_x(n, k).wait_recv()
            wo_xf(n, k).start()
            wo_d(1 + n, k).start()

    def others_first(i, carry):
        for n in range(2):
            kv2(n, i).wait_recv()
        step_a(far, i, 1, osend.at[2, i, i])
        a_relay(i).start()

        @pl.when(i == 0)
        def _():
            forward_b(1)

        def one(n, c):
            step_a(lax.rem(y + 1 + 2 * n, tp_size), i, 0, osend.at[n, i, i])
            a_direct(n, i).start()
            return c

        lax.fori_loop(0, 2, one, 0)
        for m in range(2):
            kv3(2, m, i).wait_recv()
            kv3(3, m, i).start()
        a_relay(i).wait_recv()
        a_forward(i).start()
        return carry

    lax.fori_loop(0, 2, others_first, 0)
    for k in range(3):
        for n in range(2):
            wo_xf(n, k).wait_recv()
            wo_df(n, k).start()

    def own_last(i, carry):
        for m in range(2):
            kv3(1, m, i).wait_recv()
            kv3(3, m, i).wait_recv()

        def own(s, c):
            step_a(y, i, 2, ofull.at[y, i, i, s], s)
            return c

        lax.fori_loop(0, 2, own, 0)

        @pl.when(i == 0)
        def _():
            for c in wo_local:
                c.wait()
            for k in range(3):
                for j in range(3):
                    wo_d(j, k).wait_recv()
                for n in range(2):
                    wo_df(n, k).wait_recv()

        @pl.when(i == 1)
        def _():
            forward_u(0)

        for n in range(2):
            a_direct(n, i).wait_recv()
        a_forward(i).wait_recv()
        for s in range(2):
            for n in range(2):
                b_direct(n, s, 1 - i).wait_recv()
            b_forward(s, 1 - i).wait_recv()
        for n, t in ((2, far), (0, up), (1, down), (3, y)):
            c0 = pl.multiple_of(t * cols, cols)
            acc = None
            for src in range(tp_size):
                for h in range(2):
                    lhs = ofull[src, h, i].reshape(2 * half, dim)
                    eighth = slices // 2
                    rhs = wfull[h * eighth:(h + 1) * eighth, src, :, pl.ds(c0, cols)].reshape(dim, cols)
                    res = jnp.dot(lhs, rhs, preferred_element_type=F32)
                    acc = res if acc is None else acc + res
            outsend(n, i)[...] = acc.astype(BF16)
            if n == 2:
                for r in range(2):
                    u_relay(i, r).start()
            elif n == 3:
                u_own(i).start()
            else:
                u_direct(n, i).start()
        return carry

    lax.fori_loop(0, 2, own_last, 0)
    forward_u(1)

    for c in wo_y + wo_yf:
        c.wait_send()
    for k in range(3):
        for n in range(2):
            wo_x(n, k).wait_send()
            wo_xf(n, k).wait_send()
            wo_df(n, k).wait_send()
        for j in range(3):
            wo_d(j, k).wait_send()
    for i in range(2):
        for n in range(2):
            kv2(n, i).wait_send()
            for d in (1, 2, 3):
                kv3(d, n, i).wait_send()
            a_direct(n, i).wait_send()
            for s in range(2):
                b_direct(n, s, i).wait_send()
            u_direct(n, i).wait()
            u_relay(i, n).wait_send()
            u_forward(i, n).wait()
        a_relay(i).wait_send()
        a_forward(i).wait_send()
        for s in range(2):
            b_relay(s, i).wait_send()
            b_forward(s, i).wait_send()
        u_own(i).wait()


def _natural_order(src, out):
    cols = src.shape[2]
    group = min(32, src.shape[1])
    size = group * PHASES
    to = lax.broadcasted_iota(jnp.int32, (size, size), 0)
    frm = lax.broadcasted_iota(jnp.int32, (size, size), 1)
    perm = jnp.where(frm == lax.rem(to, PHASES) * group + to // PHASES, 1.0, 0.0).astype(BF16)
    for g in range(src.shape[1] // group):
        rows = src[:, g * group:(g + 1) * group, :].reshape(size, cols)
        out[g * size:(g + 1) * size, :] = jnp.dot(perm, rows, preferred_element_type=F32).astype(BF16)


def solution(mesh):
    head_groups = mesh.shape['tp']
    seq_size = mesh.shape['sp']

    def device_fn(hidden, w_query, w_key, w_value, w_out, branch_bias):
        tokens, model_width = hidden.shape
        num_branches, num_heads = branch_bias.shape
        dim = model_width // num_heads
        local_cols = w_query.shape[1]
        cols = model_width // head_groups
        half = tokens // PHASES // 2
        block_rows = min(256, tokens // 16)
        assert head_groups == 4 and num_branches == 4 and num_heads == PHASES and local_cols == 2 * dim
        assert half * PHASES == seg_rows(tokens) and local_cols == cols
        assert 3 * model_width >= 8 * 2 * half and model_width % (2 * half) == 0
        any_spec = pl.BlockSpec(memory_space=pl.ANY)
        dma = pltpu.SemaphoreType.DMA
        tile = (half, dim)
        vm = lambda *shape: pltpu.VMEM(shape, BF16)
        phase_major = pl.pallas_call(
            functools.partial(_layer, (block_rows, half, dim, dim ** -0.5)),
            out_shape=jax.ShapeDtypeStruct((PHASES, 2 * half, cols), BF16),
            in_specs=[any_spec] * 5 + [pl.BlockSpec(memory_space=pltpu.SMEM)],
            out_specs=any_spec,
            scratch_shapes=[
                vm(2, block_rows, model_width), vm(3, model_width, local_cols),
                pltpu.VMEM((6, dim // 128, block_rows, 128), F32),
                vm(2, PHASES, 2, *tile), vm(2, PHASES, 2, *tile), vm(2, PHASES, 2, *tile),
                vm(2, 2, 2, *tile), vm(2, 2, 2, *tile), vm(3, 2, 2, *tile), vm(3, 2, 2, *tile),
                vm(seq_size, head_groups, local_cols // seq_size, model_width),
                vm(3, 2, 2, 2, *tile), vm(4, 2, 2, 2, *tile), vm(2, 2, *tile), vm(2, 2, *tile),
                vm(2, 2, half, cols),
                dma((2,)), dma((3,)), dma((seq_size,)),
                dma((2,)), dma((2,)), dma((2,)), dma((2,)), dma((2, 3)), dma((2, 3)), dma((2, 3)), dma((2, 3)),
                dma((3, 3)), dma((3, 3)), dma((2, 3)), dma((2, 3)),
                dma((2, 2)), dma((2, 2)), dma((3, 2, 2)), dma((3, 2, 2)),
                dma((2, 2)), dma((2, 2)), dma((2,)), dma((2,)), dma((2,)), dma((2,)),
                dma((2, 2, 2)), dma((2, 2, 2)), dma((2, 2)), dma((2, 2)), dma((2, 2)), dma((2, 2)),
                dma((2, 2)), dma((2, 2)), dma((2, 2)), dma((2, 2)), dma((2, 2)), dma((2, 2)), dma((2,)),
            ],
            compiler_params=pltpu.CompilerParams(collective_id=0, has_side_effects=True,
                                                 vmem_limit_bytes=67043328),
            name='layer',
        )(hidden, w_query, w_key, w_value, w_out, branch_bias)
        rows = min(128, half)
        return pl.pallas_call(
            _natural_order,
            grid=(2 * half // rows,),
            in_specs=[pl.BlockSpec((PHASES, rows, cols), lambda b: (0, b, 0))],
            out_specs=pl.BlockSpec((PHASES * rows, cols), lambda b: (b, 0)),
            out_shape=jax.ShapeDtypeStruct((tokens, cols), BF16),
            name='natural_order',
        )(phase_major)

    return jax.shard_map(device_fn, mesh=mesh, in_specs=(P(('dp', 'sp'), None), P(None, 'tp'), P(None, 'tp'), P(None, 'tp'), P('tp', None), P(None, None)), out_specs=P(('dp', 'sp'), 'tp'), check_vma=False)


def seg_rows(tokens):
    return SEG_BASE if tokens >= 2 * SEG_BASE else tokens // 2
```

```python
import functools

import jax
import jax.numpy as jnp
from jax import lax
from jax.experimental import pallas as pl
from jax.experimental.pallas import tpu as pltpu
from jax.sharding import PartitionSpec as P

SEG_BASE = 2048
PHASES = 8
SLOT = (0, 4, 2, 6, 1, 5, 3, 7)
F32 = jnp.float32
BF16 = jnp.bfloat16


def _layer(dims, hidden, wq, wk, wv, wo, bias, out, hbuf, wqkv, pf, qs, ks, vs, k2, v2, k3, v3, wfull, obuf, h_sem, w_sem, wo_loc, wy_s, wy_r, wyf_s, wyf_r, wx_s, wx_r, wxf_s, wxf_r,
           wd_s, wd_r, wdf_s, wdf_r, kv2_s, kv2_r, kv3_s, kv3_r, a_s, a_r, af_s, af_r, b_s, b_r, bf_s, bf_r, u_s, u_r,
           u_loc):
    block_rows, half, dim, scale = dims
    tp_size = 4
    y = lax.axis_index('tp')
    sp = lax.axis_index('sp')
    up = lax.rem(y + 1, tp_size)
    far = lax.rem(y + 2, tp_size)
    down = lax.rem(y + 3, tp_size)
    tokens = hidden.shape[0]
    num_blocks = tokens // block_rows
    half_blocks = num_blocks // 2
    phase_rows = block_rows // PHASES
    slices, _, piece, _ = wfull.shape
    cols = wqkv.shape[2]

    def sp_peer(dist):
        base = (sp // 4) * 4
        pos = lax.rem(sp, 4)
        if dist == 1:
            other = pos + 1 - 2 * lax.rem(pos, 2)
        elif dist == 2:
            other = lax.rem(pos + 2, 4)
        else:
            other = 3 - pos
        return base + other

    partner = sp_peer(1)
    right = lax.rem(sp + 2, slices)
    opposite = lax.rem(sp + slices // 2, slices)
    left = lax.rem(sp + slices - 2, slices)

    def remote(src, dst, ssem, rsem, dev):
        return pltpu.make_async_remote_copy(src_ref=src, dst_ref=dst, send_sem=ssem, recv_sem=rsem, device_id=dev,
                                            device_id_type=pl.DeviceIdType.MESH)

    def load_hidden(b):
        slot = lax.rem(b, 2)
        return pltpu.make_async_copy(hidden.at[pl.ds(b * block_rows, block_rows), :], hbuf.at[slot], h_sem.at[slot])

    w_loads = [pltpu.make_async_copy(w, wqkv.at[n], w_sem.at[n]) for n, w in enumerate((wq, wk, wv))]
    load_hidden(0).start()
    w_loads[0].start()
    w_loads[1].start()
    w_loads[2].start()
    wo_local = [pltpu.make_async_copy(wo.at[pl.ds(j * piece, piece), :], wfull.at[j, y], wo_loc.at[j])
                for j in range(slices)]
    barrier = pltpu.get_barrier_semaphore()
    peers = [{'tp': up}, {'tp': far}, {'tp': down}, {'sp': partner}, {'sp': right}, {'sp': left}]
    for dev in peers:
        pl.semaphore_signal(barrier, inc=1, device_id=dev, device_id_type=pl.DeviceIdType.MESH)

    dirs = (up, down)
    near = (down, up)
    xdirs = (right, left)
    xnear = (left, right)
    part = [pl.ds(0, piece // 2), pl.ds(piece // 2, piece // 2)]
    wo_y = [remote(wo.at[pl.ds(pl.multiple_of(sp * piece, piece), piece), :], wfull.at[sp, y], wy_s.at[n], wy_r.at[n],
                   {'tp': dirs[n]}) for n in range(2)]
    wo_yf = [remote(wfull.at[sp, near[n], part[n]], wfull.at[sp, near[n], part[n]], wyf_s.at[n], wyf_r.at[n],
                    {'tp': dirs[n]}) for n in range(2)]
    others = (up, far, down)

    def wo_x(n, k):
        ref = wfull.at[sp, others[k]]
        return remote(ref, ref, wx_s.at[n, k], wx_r.at[n, k], {'sp': xdirs[n]})

    def wo_xf(n, k):
        ref = wfull.at[xnear[n], others[k], part[n]]
        return remote(ref, ref, wxf_s.at[n, k], wxf_r.at[n, k], {'sp': xdirs[n]})

    def wo_d(j, k):
        ref = wfull.at[(sp, left, right)[j], others[k]]
        return remote(ref, ref, wd_s.at[j, k], wd_r.at[j, k], {'sp': partner})

    def wo_df(n, k):
        ref = wfull.at[opposite, others[k], part[n]]
        return remote(ref, ref, wdf_s.at[n, k], wdf_r.at[n, k], {'sp': partner})

    u_y = lax.rem(y, 2) * 2 + y // 2
    pair_y = lax.rem(y, 2) * 2
    kv = ((ks, k2, k3), (vs, v2, v3))

    def kv2(n, i):
        src, two, _ = kv[n]
        return remote(src.at[i, pl.ds(4 * i + pair_y, 2)], two.at[i], kv2_s.at[n, i], kv2_r.at[n, i], {'sp': partner})

    def kv3(d, n, i):
        src, _, three = kv[n]
        ref = three.at[1, i] if d == 3 else src.at[i, 4 * i + u_y]
        return remote(ref, three.at[d - 1, i], kv3_s.at[d - 1, n, i], kv3_r.at[d - 1, n, i],
                      {'sp': partner if d == 3 else sp_peer(d)})

    def attend(q, keys, values, after=None):
        if after is not None:
            q = q + jnp.minimum(after, 0.0).astype(BF16)
        logits = [lax.dot_general(q, k, (((1,), (1,)), ((), ())), preferred_element_type=F32) for k in keys]
        top = logits[0]
        for x in logits[1:]:
            top = jnp.maximum(top, x)
        top = jnp.max(top, axis=1, keepdims=True)
        total = None
        numer = None
        for x, v in zip(logits, values):
            e = jnp.exp(x - top)
            total = e if total is None else total + e
            piece_sum = jnp.dot(e.astype(BF16), v, preferred_element_type=F32)
            numer = piece_sum if numer is None else numer + piece_sum
        return numer, top, jnp.sum(total, axis=1, keepdims=True)

    def slot_of(t):
        return lax.rem(t, 2) * 2 + t // 2

    def step_b(s, i, t0, t1, dst0, dst1, after=None):
        q = jnp.concatenate([qs[i, 4 * (1 - i) + slot_of(t0), s], qs[i, 4 * (1 - i) + slot_of(t1), s]], axis=0)
        n, _, l = attend(q, [ks[i, c, s] for c in range(PHASES)], [vs[i, c, s] for c in range(PHASES)], after)
        o = (n / l).astype(BF16)
        dst0[...] = o[:half]
        dst1[...] = o[half:]
        return l

    def step_a(t, i, level, dst, s=None):
        slot = 4 * i + slot_of(t)
        zero = [attend(qs[i, slot, h], [ks[i, c, h] for c in range(PHASES)], [vs[i, c, h] for c in range(PHASES)])
                for h in (range(2) if s is None else (s,))]
        if s is None:
            parts = [tuple(jnp.concatenate([a, b], axis=0) for a, b in zip(*zero))]
            q = qs[i, slot].reshape(2 * half, dim)
        else:
            parts = zero
            q = qs[i, slot, s]
        tiles = [(4 * i + c, h) for c in range(4) for h in range(2)]
        parts.append(attend(q, [ks[i, c, h] for c, h in tiles], [vs[i, c, h] for c, h in tiles]))
        if level >= 1:
            tiles = [(c, h) for c in range(2) for h in range(2)]
            base = 4 * i + pair_y
            parts.append(attend(q, [ks[i, base + c, h] for c, h in tiles] + [k2[i, c, h] for c, h in tiles],
                                [vs[i, base + c, h] for c, h in tiles] + [v2[i, c, h] for c, h in tiles]))
        if level >= 2:
            mine = 4 * i + u_y
            tiles = [(d, h) for d in range(3) for h in range(2)]
            parts.append(attend(q, [ks[i, mine, h] for h in range(2)] + [k3[d, i, h] for d, h in tiles],
                                [vs[i, mine, h] for h in range(2)] + [v3[d, i, h] for d, h in tiles]))
        scores = [m + bias[j, 2 * y + i] for j, (_, m, _) in enumerate(parts)]
        best = functools.reduce(jnp.maximum, scores)
        num = None
        den = None
        for (n, _, l), sc in zip(parts, scores):
            w = jnp.exp(sc - best)
            num = n * w if num is None else num + n * w
            den = l * w if den is None else den + l * w
        dst[...] = (num / den).astype(BF16).reshape(dst.shape)

    def flow(f):
        return ((8, y, up), (9, 4 + y, down), (4 + y, y, down), (y, 4 + y, up))[f]

    def send_a(f, i):
        here, there, dev = flow(f)
        return remote(obuf.at[here, i, i], obuf.at[there, i, i], a_s.at[f, i], a_r.at[f, i], {'tp': dev})

    def send_b(f, s, i):
        here, there, dev = flow(f)
        return remote(obuf.at[here, i, 1 - i, s], obuf.at[there, i, 1 - i, s], b_s.at[f, s, i], b_r.at[f, s, i],
                      {'tp': dev})

    def onward(n):
        return ((down, 4 + down, up), (4 + up, up, down))[n]

    def pass_a(n, i):
        here, there, dev = onward(n)
        return remote(obuf.at[here, i, i], obuf.at[there, i, i], af_s.at[n, i], af_r.at[n, i], {'tp': dev})

    def pass_b(n, s, i):
        here, there, dev = onward(n)
        return remote(obuf.at[here, i, 1 - i, s], obuf.at[there, i, 1 - i, s], bf_s.at[n, s, i], bf_r.at[n, s, i],
                      {'tp': dev})

    def forward_a(i):
        for n in range(2):
            send_a(n, i).wait_recv()
            pass_a(n, i).start()

    def forward_b(s):
        for i in range(2):
            for n in range(2):
                send_b(n, s, i).wait_recv()
                pass_b(n, s, i).start()

    for c in w_loads:
        c.wait()

    def place(buf, n, i, b):
        r0 = pl.multiple_of(lax.rem(b, half_blocks) * phase_rows, phase_rows)
        for g in range(dim // 128):
            for ph in range(PHASES):
                picked = buf[g, pl.ds(ph, phase_rows, stride=PHASES), :]
                kv_q[n][i, SLOT[ph], b // half_blocks, pl.ds(r0, phase_rows), g * 128:(g + 1) * 128] = picked.astype(BF16)

    def place_last(b):
        place(pf.at[4 + lax.rem(b, 2)], 2, 1, b)

    kv_q = (qs, ks, vs)

    def first(s, carry):
        def project(r, c):
            b = s * half_blocks + r
            load_hidden(b).wait()

            @pl.when(b + 1 < num_blocks)
            def _():
                load_hidden(b + 1).start()

            @pl.when(b == 1)
            def _():
                pl.semaphore_wait(barrier, len(peers))
                for c in wo_y + wo_local:
                    c.start()

            @pl.when(b == half_blocks - 2)
            def _():
                for n in range(2):
                    wo_y[n].wait_recv()
                    wo_yf[n].start()

            @pl.when(b == half_blocks + 1)
            def _():
                for c in wo_yf:
                    c.wait_recv()
                for k in range(3):
                    for n in range(2):
                        wo_x(n, k).start()
                    wo_d(0, k).start()

            @pl.when(b == num_blocks - 2)
            def _():
                forward_b(0)

            rows = hbuf[lax.rem(b, 2)]
            place_last(jnp.maximum(b - 1, 0))
            for n in range(3):
                for i in range(2):
                    res = jnp.dot(rows, wqkv[n, :, i * dim:(i + 1) * dim], preferred_element_type=F32)
                    if n == 0:
                        res = res * scale
                    piece_no = n * 2 + i
                    buf = pf.at[4 + lax.rem(b, 2) if piece_no == 5 else piece_no % 4]
                    for g in range(dim // 128):
                        buf[g] = res[:, g * 128:(g + 1) * 128]
                    if piece_no < 5:
                        place(buf, n, i, b)
            return c

        lax.fori_loop(0, half_blocks, project, 0)
        place_last((s + 1) * half_blocks - 1)

        @pl.when(s == 1)
        def _():
            for i in range(2):
                for n in range(2):
                    kv2(n, i).start()
                    for d in (2, 1):
                        kv3(d, n, i).start()

        sums = (None, None)
        for i in range(2):
            sums = (step_b(s, i, far, y, obuf.at[9, i, 1 - i, s], obuf.at[y, i, 1 - i, s], sums[0]),
                    step_b(s, i, up, down, obuf.at[8, i, 1 - i, s], obuf.at[4 + y, i, 1 - i, s], sums[1]))
        for i in range(2):
            for f in range(4):
                send_b(f, s, i).start()
        return carry

    lax.fori_loop(0, 2, first, 0)

    for k in range(3):
        for n in range(2):
            wo_x(n, k).wait_recv()
            wo_xf(n, k).start()
            wo_d(1 + n, k).start()

    def others_first(i, carry):
        for n in range(2):
            kv2(n, i).wait_recv()
        step_a(far, i, 1, obuf.at[9, i, i])
        send_a(1, i).start()

        @pl.when(i == 1)
        def _():
            forward_a(0)

        def one(n, c):
            step_a(lax.rem(y + 1 + 2 * n, tp_size), i, 0, obuf.at[8 + n * (y - 4), i, i])

            @pl.when(n == 0)
            def _():
                send_a(0, i).start()

            @pl.when(n == 1)
            def _():
                send_a(2, i).start()
            return c

        lax.fori_loop(0, 2, one, 0)

        @pl.when(i == 0)
        def _():
            forward_b(1)

        for m in range(2):
            kv3(2, m, i).wait_recv()
            kv3(3, m, i).start()
        return carry

    lax.fori_loop(0, 2, others_first, 0)
    for k in range(3):
        for n in range(2):
            wo_xf(n, k).wait_recv()
            wo_df(n, k).start()

    def own_last(i, carry):
        for m in range(2):
            kv3(1, m, i).wait_recv()
            kv3(3, m, i).wait_recv()

        @pl.when(i == 1)
        def _():
            forward_a(1)

        def own(s, c):
            step_a(y, i, 2, obuf.at[y, i, i, s], s)
            return c

        lax.fori_loop(0, 2, own, 0)
        send_a(3, i).start()
        return carry

    lax.fori_loop(0, 2, own_last, 0)

    for c in wo_local:
        c.wait()
    for k in range(3):
        for j in range(3):
            wo_d(j, k).wait_recv()
        for n in range(2):
            wo_df(n, k).wait_recv()

    def result(g, kind, i):
        k = 4 * g + 2 * kind + i
        per = wqkv.shape[1] // (2 * half)
        return wqkv.at[k // per, pl.ds(pl.multiple_of(lax.rem(k, per) * 2 * half, 2 * half), 2 * half), :]

    def u_send(g, i):
        return remote(result(g, 0, i), out.at[2 * (y, down)[g] + i], u_s.at[g, i], u_r.at[g, i],
                      {'tp': (down, up)[g]})

    def u_own(g, i):
        return pltpu.make_async_copy(result(g, 1, i), out.at[2 * (y, down)[g] + i], u_loc.at[g, i])

    def project_out(i, carry):
        for g in range(2):
            send_a((2, 3)[g], i).wait_recv()
            pass_a(1 - g, i).wait_recv()
            for s in range(2):
                send_b((2, 3)[g], s, 1 - i).wait_recv()
                pass_b(1 - g, s, 1 - i).wait_recv()
            for kind, t in enumerate(((down, up)[g], y)):
                c0 = pl.multiple_of(t * cols, cols)
                acc = None
                for src in range(tp_size):
                    for h in range(2):
                        lhs = obuf[4 * g + src, h, i].reshape(2 * half, dim)
                        eighth = slices // 2
                        rhs = wfull[h * eighth:(h + 1) * eighth, src, :, pl.ds(c0, cols)].reshape(dim, cols)
                        res = jnp.dot(lhs, rhs, preferred_element_type=F32)
                        acc = res if acc is None else acc + res
                result(g, kind, i)[...] = acc.astype(BF16)
                (u_send, u_own)[kind](g, i).start()
        return carry

    lax.fori_loop(0, 2, project_out, 0)

    for c in wo_y + wo_yf:
        c.wait_send()
    for k in range(3):
        for n in range(2):
            wo_x(n, k).wait_send()
            wo_xf(n, k).wait_send()
            wo_df(n, k).wait_send()
        for j in range(3):
            wo_d(j, k).wait_send()
    for i in range(2):
        for n in range(2):
            kv2(n, i).wait_send()
            for d in (1, 2, 3):
                kv3(d, n, i).wait_send()
            pass_a(n, i).wait_send()
            for s in range(2):
                pass_b(n, s, i).wait_send()
            u_send(n, i).wait()
            u_own(n, i).wait()
        for f in range(4):
            send_a(f, i).wait_send()
            for s in range(2):
                send_b(f, s, i).wait_send()


def _natural_order(src, out):
    cols = src.shape[2]
    group = min(32, src.shape[1])
    size = group * PHASES
    to = lax.broadcasted_iota(jnp.int32, (size, size), 0)
    frm = lax.broadcasted_iota(jnp.int32, (size, size), 1)
    perm = jnp.where(frm == lax.rem(to, PHASES) * group + to // PHASES, 1.0, 0.0).astype(BF16)
    for g in range(src.shape[1] // group):
        rows = src[:, g * group:(g + 1) * group, :].reshape(size, cols)
        out[g * size:(g + 1) * size, :] = jnp.dot(perm, rows, preferred_element_type=F32).astype(BF16)


def solution(mesh):
    head_groups = mesh.shape['tp']
    seq_size = mesh.shape['sp']

    def device_fn(hidden, w_query, w_key, w_value, w_out, branch_bias):
        tokens, model_width = hidden.shape
        num_branches, num_heads = branch_bias.shape
        dim = model_width // num_heads
        local_cols = w_query.shape[1]
        cols = model_width // head_groups
        half = tokens // PHASES // 2
        block_rows = min(256, tokens // 16)
        assert head_groups == 4 and num_branches == 4 and num_heads == PHASES and local_cols == 2 * dim
        assert half * PHASES == seg_rows(tokens) and local_cols == cols
        assert 3 * model_width >= 8 * 2 * half and model_width % (2 * half) == 0
        any_spec = pl.BlockSpec(memory_space=pl.ANY)
        dma = pltpu.SemaphoreType.DMA
        tile = (half, dim)
        vm = lambda *shape: pltpu.VMEM(shape, BF16)
        phase_major = pl.pallas_call(
            functools.partial(_layer, (block_rows, half, dim, dim ** -0.5)),
            out_shape=jax.ShapeDtypeStruct((PHASES, 2 * half, cols), BF16),
            in_specs=[any_spec] * 5 + [pl.BlockSpec(memory_space=pltpu.SMEM)],
            out_specs=any_spec,
            scratch_shapes=[
                vm(2, block_rows, model_width), vm(3, model_width, local_cols),
                pltpu.VMEM((6, dim // 128, block_rows, 128), F32),
                vm(2, PHASES, 2, *tile), vm(2, PHASES, 2, *tile), vm(2, PHASES, 2, *tile),
                vm(2, 2, 2, *tile), vm(2, 2, 2, *tile), vm(3, 2, 2, *tile), vm(3, 2, 2, *tile),
                vm(seq_size, head_groups, local_cols // seq_size, model_width),
                vm(10, 2, 2, 2, *tile),
                dma((2,)), dma((3,)), dma((seq_size,)),
                dma((2,)), dma((2,)), dma((2,)), dma((2,)), dma((2, 3)), dma((2, 3)), dma((2, 3)), dma((2, 3)),
                dma((3, 3)), dma((3, 3)), dma((2, 3)), dma((2, 3)),
                dma((2, 2)), dma((2, 2)), dma((3, 2, 2)), dma((3, 2, 2)),
                dma((4, 2)), dma((4, 2)), dma((2, 2)), dma((2, 2)), dma((4, 2, 2)), dma((4, 2, 2)), dma((2, 2, 2)),
                dma((2, 2, 2)), dma((2, 2)), dma((2, 2)), dma((2, 2)),
            ],
            compiler_params=pltpu.CompilerParams(collective_id=0, has_side_effects=True,
                                                 vmem_limit_bytes=67043328),
            name='layer',
        )(hidden, w_query, w_key, w_value, w_out, branch_bias)
        rows = min(128, half)
        return pl.pallas_call(
            _natural_order,
            grid=(2 * half // rows,),
            in_specs=[pl.BlockSpec((PHASES, rows, cols), lambda b: (0, b, 0))],
            out_specs=pl.BlockSpec((PHASES * rows, cols), lambda b: (b, 0)),
            out_shape=jax.ShapeDtypeStruct((tokens, cols), BF16),
            name='natural_order',
        )(phase_major)

    return jax.shard_map(device_fn, mesh=mesh, in_specs=(P(('dp', 'sp'), None), P(None, 'tp'), P(None, 'tp'), P(None, 'tp'), P('tp', None), P(None, None)), out_specs=P(('dp', 'sp'), 'tp'), check_vma=False)


def seg_rows(tokens):
    return SEG_BASE if tokens >= 2 * SEG_BASE else tokens // 2
```

```python
import functools

import jax
import jax.numpy as jnp
from jax import lax
from jax.experimental import pallas as pl
from jax.experimental.pallas import tpu as pltpu
from jax.sharding import PartitionSpec as P

SEG_BASE = 2048
PHASES = 8
SLOT = (0, 4, 2, 6, 1, 5, 3, 7)
F32 = jnp.float32
BF16 = jnp.bfloat16


def _layer(dims, hidden, wq, wk, wv, wo, bias, out, hbuf, wqkv, pf, qs, ks, vs, k2, v2, k3, v3, wfull, obuf, h_sem, w_sem, wo_loc, wy_s, wy_r, wyf_s, wyf_r, wx_s, wx_r, wxf_s, wxf_r,
           wd_s, wd_r, wdf_s, wdf_r, kv2_s, kv2_r, kv3_s, kv3_r, a_s, a_r, af_s, af_r, b_s, b_r, bf_s, bf_r, u_s, u_r,
           u_loc):
    block_rows, half, dim, scale = dims
    tp_size = 4
    y = lax.axis_index('tp')
    sp = lax.axis_index('sp')
    up = lax.rem(y + 1, tp_size)
    far = lax.rem(y + 2, tp_size)
    down = lax.rem(y + 3, tp_size)
    tokens = hidden.shape[0]
    num_blocks = tokens // block_rows
    half_blocks = num_blocks // 2
    phase_rows = block_rows // PHASES
    slices, _, piece, _ = wfull.shape
    cols = wqkv.shape[2]

    def sp_peer(dist):
        base = (sp // 4) * 4
        pos = lax.rem(sp, 4)
        if dist == 1:
            other = pos + 1 - 2 * lax.rem(pos, 2)
        elif dist == 2:
            other = lax.rem(pos + 2, 4)
        else:
            other = 3 - pos
        return base + other

    partner = sp_peer(1)
    right = lax.rem(sp + 2, slices)
    opposite = lax.rem(sp + slices // 2, slices)
    left = lax.rem(sp + slices - 2, slices)

    def remote(src, dst, ssem, rsem, dev):
        return pltpu.make_async_remote_copy(src_ref=src, dst_ref=dst, send_sem=ssem, recv_sem=rsem, device_id=dev,
                                            device_id_type=pl.DeviceIdType.MESH)

    def load_hidden(b):
        slot = lax.rem(b, 2)
        return pltpu.make_async_copy(hidden.at[pl.ds(b * block_rows, block_rows), :], hbuf.at[slot], h_sem.at[slot])

    w_loads = [pltpu.make_async_copy(w, wqkv.at[n], w_sem.at[n]) for n, w in enumerate((wq, wk, wv))]
    load_hidden(0).start()
    w_loads[0].start()
    w_loads[1].start()
    w_loads[2].start()
    wo_local = [pltpu.make_async_copy(wo.at[pl.ds(j * piece, piece), :], wfull.at[j, y], wo_loc.at[j])
                for j in range(slices)]
    barrier = pltpu.get_barrier_semaphore()
    peers = [{'tp': up}, {'tp': far}, {'tp': down}, {'sp': partner}, {'sp': right}, {'sp': left}]
    for dev in peers:
        pl.semaphore_signal(barrier, inc=1, device_id=dev, device_id_type=pl.DeviceIdType.MESH)

    dirs = (up, down)
    near = (down, up)
    xdirs = (right, left)
    xnear = (left, right)
    part = [pl.ds(0, piece // 2), pl.ds(piece // 2, piece // 2)]
    wo_y = [remote(wo.at[pl.ds(pl.multiple_of(sp * piece, piece), piece), :], wfull.at[sp, y], wy_s.at[n], wy_r.at[n],
                   {'tp': dirs[n]}) for n in range(2)]
    wo_yf = [remote(wfull.at[sp, near[n], part[n]], wfull.at[sp, near[n], part[n]], wyf_s.at[n], wyf_r.at[n],
                    {'tp': dirs[n]}) for n in range(2)]
    others = (up, far, down)

    def wo_x(n, k):
        ref = wfull.at[sp, others[k]]
        return remote(ref, ref, wx_s.at[n, k], wx_r.at[n, k], {'sp': xdirs[n]})

    def wo_xf(n, k):
        ref = wfull.at[xnear[n], others[k], part[n]]
        return remote(ref, ref, wxf_s.at[n, k], wxf_r.at[n, k], {'sp': xdirs[n]})

    def wo_d(j, k):
        ref = wfull.at[(sp, left, right)[j], others[k]]
        return remote(ref, ref, wd_s.at[j, k], wd_r.at[j, k], {'sp': partner})

    def wo_df(n, k):
        ref = wfull.at[opposite, others[k], part[n]]
        return remote(ref, ref, wdf_s.at[n, k], wdf_r.at[n, k], {'sp': partner})

    u_y = lax.rem(y, 2) * 2 + y // 2
    pair_y = lax.rem(y, 2) * 2
    kv = ((ks, k2, k3), (vs, v2, v3))

    def kv2(n, i):
        src, two, _ = kv[n]
        return remote(src.at[i, pl.ds(4 * i + pair_y, 2)], two.at[i], kv2_s.at[n, i], kv2_r.at[n, i], {'sp': partner})

    def kv3(d, n, i):
        src, _, three = kv[n]
        ref = three.at[1, i] if d == 3 else src.at[i, 4 * i + u_y]
        return remote(ref, three.at[d - 1, i], kv3_s.at[d - 1, n, i], kv3_r.at[d - 1, n, i],
                      {'sp': partner if d == 3 else sp_peer(d)})

    def attend(q, keys, values, after=None):
        if after is not None:
            q = q + jnp.minimum(after, 0.0).astype(BF16)
        logits = [lax.dot_general(q, k, (((1,), (1,)), ((), ())), preferred_element_type=F32) for k in keys]
        top = logits[0]
        for x in logits[1:]:
            top = jnp.maximum(top, x)
        top = jnp.max(top, axis=1, keepdims=True)
        total = None
        numer = None
        for x, v in zip(logits, values):
            e = jnp.exp(x - top)
            total = e if total is None else total + e
            piece_sum = jnp.dot(e.astype(BF16), v, preferred_element_type=F32)
            numer = piece_sum if numer is None else numer + piece_sum
        return numer, top, jnp.sum(total, axis=1, keepdims=True)

    def slot_of(t):
        return lax.rem(t, 2) * 2 + t // 2

    def step_b(s, i, t0, t1, dst0, dst1, after=None):
        q = jnp.concatenate([qs[i, 4 * (1 - i) + slot_of(t0), s], qs[i, 4 * (1 - i) + slot_of(t1), s]], axis=0)
        n, _, l = attend(q, [ks[i, c, s] for c in range(PHASES)], [vs[i, c, s] for c in range(PHASES)], after)
        o = (n / l).astype(BF16)
        dst0[...] = o[:half]
        dst1[...] = o[half:]
        return l

    def step_a(t, i, level, dst, s=None):
        slot = 4 * i + slot_of(t)
        zero = [attend(qs[i, slot, h], [ks[i, c, h] for c in range(PHASES)], [vs[i, c, h] for c in range(PHASES)])
                for h in (range(2) if s is None else (s,))]
        if s is None:
            parts = [tuple(jnp.concatenate([a, b], axis=0) for a, b in zip(*zero))]
            q = qs[i, slot].reshape(2 * half, dim)
        else:
            parts = zero
            q = qs[i, slot, s]
        tiles = [(4 * i + c, h) for c in range(4) for h in range(2)]
        parts.append(attend(q, [ks[i, c, h] for c, h in tiles], [vs[i, c, h] for c, h in tiles]))
        if level >= 1:
            tiles = [(c, h) for c in range(2) for h in range(2)]
            base = 4 * i + pair_y
            parts.append(attend(q, [ks[i, base + c, h] for c, h in tiles] + [k2[i, c, h] for c, h in tiles],
                                [vs[i, base + c, h] for c, h in tiles] + [v2[i, c, h] for c, h in tiles]))
        if level >= 2:
            mine = 4 * i + u_y
            tiles = [(d, h) for d in range(3) for h in range(2)]
            parts.append(attend(q, [ks[i, mine, h] for h in range(2)] + [k3[d, i, h] for d, h in tiles],
                                [vs[i, mine, h] for h in range(2)] + [v3[d, i, h] for d, h in tiles]))
        scores = [m + bias[j, 2 * y + i] for j, (_, m, _) in enumerate(parts)]
        best = functools.reduce(jnp.maximum, scores)
        num = None
        den = None
        for (n, _, l), sc in zip(parts, scores):
            w = jnp.exp(sc - best)
            num = n * w if num is None else num + n * w
            den = l * w if den is None else den + l * w
        dst[...] = (num / den).astype(BF16).reshape(dst.shape)

    def flow(f):
        return ((8, y, up), (9, 4 + y, down), (4 + y, y, down), (y, 4 + y, up))[f]

    def send_a(f, i):
        here, there, dev = flow(f)
        return remote(obuf.at[here, i, i], obuf.at[there, i, i], a_s.at[f, i], a_r.at[f, i], {'tp': dev})

    def send_b(f, s, i):
        here, there, dev = flow(f)
        return remote(obuf.at[here, i, 1 - i, s], obuf.at[there, i, 1 - i, s], b_s.at[f, s, i], b_r.at[f, s, i],
                      {'tp': dev})

    def onward(n):
        return ((down, 4 + down, up), (4 + up, up, down))[n]

    def pass_a(n, i):
        here, there, dev = onward(n)
        return remote(obuf.at[here, i, i], obuf.at[there, i, i], af_s.at[n, i], af_r.at[n, i], {'tp': dev})

    def pass_b(n, s, i):
        here, there, dev = onward(n)
        return remote(obuf.at[here, i, 1 - i, s], obuf.at[there, i, 1 - i, s], bf_s.at[n, s, i], bf_r.at[n, s, i],
                      {'tp': dev})

    def forward_a(i):
        for n in range(2):
            send_a(n, i).wait_recv()
            pass_a(n, i).start()

    def forward_b(s):
        for i in range(2):
            for n in range(2):
                send_b(n, s, i).wait_recv()
                pass_b(n, s, i).start()

    for c in w_loads:
        c.wait()

    def place(buf, n, i, b):
        r0 = pl.multiple_of(lax.rem(b, half_blocks) * phase_rows, phase_rows)
        for g in range(dim // 128):
            for ph in range(PHASES):
                picked = buf[g, pl.ds(ph, phase_rows, stride=PHASES), :]
                kv_q[n][i, SLOT[ph], b // half_blocks, pl.ds(r0, phase_rows), g * 128:(g + 1) * 128] = picked.astype(BF16)

    def place_last(b):
        place(pf.at[4 + lax.rem(b, 2)], 2, 1, b)

    kv_q = (qs, ks, vs)

    def first(s, carry):
        def project(r, c):
            b = s * half_blocks + r
            load_hidden(b).wait()

            @pl.when(b + 1 < num_blocks)
            def _():
                load_hidden(b + 1).start()

            @pl.when(b == 1)
            def _():
                pl.semaphore_wait(barrier, len(peers))
                for c in wo_y + wo_local:
                    c.start()

            @pl.when(b == half_blocks - 2)
            def _():
                for n in range(2):
                    wo_y[n].wait_recv()
                    wo_yf[n].start()

            @pl.when(b == half_blocks + 1)
            def _():
                for c in wo_yf:
                    c.wait_recv()
                for k in range(3):
                    for n in range(2):
                        wo_x(n, k).start()
                    wo_d(0, k).start()

            @pl.when(b == num_blocks - 2)
            def _():
                forward_b(0)

            rows = hbuf[lax.rem(b, 2)]
            place_last(jnp.maximum(b - 1, 0))
            for n in range(3):
                for i in range(2):
                    res = jnp.dot(rows, wqkv[n, :, i * dim:(i + 1) * dim], preferred_element_type=F32)
                    if n == 0:
                        res = res * scale
                    piece_no = n * 2 + i
                    buf = pf.at[4 + lax.rem(b, 2) if piece_no == 5 else piece_no % 4]
                    for g in range(dim // 128):
                        buf[g] = res[:, g * 128:(g + 1) * 128]
                    if piece_no < 5:
                        place(buf, n, i, b)
            return c

        lax.fori_loop(0, half_blocks, project, 0)
        place_last((s + 1) * half_blocks - 1)

        @pl.when(s == 1)
        def _():
            for i in range(2):
                for n in range(2):
                    kv2(n, i).start()
                    for d in (2, 1):
                        kv3(d, n, i).start()

        sums = (None, None)
        for i in range(2):
            sums = (step_b(s, i, far, y, obuf.at[9, i, 1 - i, s], obuf.at[y, i, 1 - i, s], sums[0]),
                    step_b(s, i, up, down, obuf.at[8, i, 1 - i, s], obuf.at[4 + y, i, 1 - i, s], sums[1]))
        for fs in ((0, 1), (2, 3)):
            for i in range(2):
                for f in fs:
                    send_b(f, s, i).start()
        return carry

    lax.fori_loop(0, 2, first, 0)

    for k in range(3):
        for n in range(2):
            wo_x(n, k).wait_recv()
            wo_xf(n, k).start()
            wo_d(1 + n, k).start()

    def others_first(i, carry):
        for n in range(2):
            kv2(n, i).wait_recv()
        step_a(far, i, 1, obuf.at[9, i, i])
        send_a(1, i).start()

        @pl.when(i == 1)
        def _():
            forward_a(0)

        def one(n, c):
            step_a(lax.rem(y + 1 + 2 * n, tp_size), i, 0, obuf.at[8 + n * (y - 4), i, i])

            @pl.when(n == 0)
            def _():
                send_a(0, i).start()

            @pl.when(n == 1)
            def _():
                send_a(2, i).start()
            return c

        lax.fori_loop(0, 2, one, 0)

        @pl.when(i == 0)
        def _():
            forward_b(1)

        for m in range(2):
            kv3(2, m, i).wait_recv()
            kv3(3, m, i).start()
        return carry

    lax.fori_loop(0, 2, others_first, 0)
    for k in range(3):
        for n in range(2):
            wo_xf(n, k).wait_recv()
            wo_df(n, k).start()

    def own_last(i, carry):
        for m in range(2):
            kv3(1, m, i).wait_recv()
            kv3(3, m, i).wait_recv()

        @pl.when(i == 1)
        def _():
            forward_a(1)

        def own(s, c):
            step_a(y, i, 2, obuf.at[y, i, i, s], s)
            return c

        lax.fori_loop(0, 2, own, 0)
        send_a(3, i).start()
        return carry

    lax.fori_loop(0, 2, own_last, 0)

    for c in wo_local:
        c.wait()
    for k in range(3):
        for j in range(3):
            wo_d(j, k).wait_recv()
        for n in range(2):
            wo_df(n, k).wait_recv()

    def result(g, kind, i):
        k = 4 * g + 2 * kind + i
        per = wqkv.shape[1] // (2 * half)
        return wqkv.at[k // per, pl.ds(pl.multiple_of(lax.rem(k, per) * 2 * half, 2 * half), 2 * half), :]

    def u_send(g, i):
        return remote(result(g, 0, i), out.at[2 * (y, down)[g] + i], u_s.at[g, i], u_r.at[g, i],
                      {'tp': (down, up)[g]})

    def u_own(g, i):
        return pltpu.make_async_copy(result(g, 1, i), out.at[2 * (y, down)[g] + i], u_loc.at[g, i])

    def project_out(i, carry):
        for g in range(2):
            send_a((2, 3)[g], i).wait_recv()
            pass_a(1 - g, i).wait_recv()
            for s in range(2):
                send_b((2, 3)[g], s, 1 - i).wait_recv()
                pass_b(1 - g, s, 1 - i).wait_recv()
            for kind, t in enumerate(((down, up)[g], y)):
                c0 = pl.multiple_of(t * cols, cols)
                acc = None
                for src in range(tp_size):
                    for h in range(2):
                        lhs = obuf[4 * g + src, h, i].reshape(2 * half, dim)
                        eighth = slices // 2
                        rhs = wfull[h * eighth:(h + 1) * eighth, src, :, pl.ds(c0, cols)].reshape(dim, cols)
                        res = jnp.dot(lhs, rhs, preferred_element_type=F32)
                        acc = res if acc is None else acc + res
                result(g, kind, i)[...] = acc.astype(BF16)
                (u_send, u_own)[kind](g, i).start()
        return carry

    lax.fori_loop(0, 2, project_out, 0)

    for c in wo_y + wo_yf:
        c.wait_send()
    for k in range(3):
        for n in range(2):
            wo_x(n, k).wait_send()
            wo_xf(n, k).wait_send()
            wo_df(n, k).wait_send()
        for j in range(3):
            wo_d(j, k).wait_send()
    for i in range(2):
        for n in range(2):
            kv2(n, i).wait_send()
            for d in (1, 2, 3):
                kv3(d, n, i).wait_send()
            pass_a(n, i).wait_send()
            for s in range(2):
                pass_b(n, s, i).wait_send()
            u_send(n, i).wait()
            u_own(n, i).wait()
        for f in range(4):
            send_a(f, i).wait_send()
            for s in range(2):
                send_b(f, s, i).wait_send()


def _natural_order(src, out, rows_in, rows_out, in_sem, out_sem):
    cols = src.shape[2]
    per = src.shape[1] // in_sem.shape[0]
    group = min(32, per)
    size = group * PHASES
    loads = [pltpu.make_async_copy(src.at[:, pl.ds(c * per, per), :], rows_in.at[:, pl.ds(c * per, per), :],
                                   in_sem.at[c]) for c in range(in_sem.shape[0])]
    stores = [pltpu.make_async_copy(rows_out.at[pl.ds(c * per * PHASES, per * PHASES), :],
                                    out.at[pl.ds(c * per * PHASES, per * PHASES), :], out_sem.at[c])
              for c in range(out_sem.shape[0])]
    for c in loads:
        c.start()
    to = lax.broadcasted_iota(jnp.int32, (size, size), 0)
    frm = lax.broadcasted_iota(jnp.int32, (size, size), 1)
    perm = jnp.where(frm == lax.rem(to, PHASES) * group + to // PHASES, 1.0, 0.0).astype(BF16)
    for c in range(in_sem.shape[0]):
        loads[c].wait()
        for g in range(c * per, (c + 1) * per, group):
            rows = rows_in[:, g:g + group, :].reshape(size, cols)
            rows_out[g * PHASES:g * PHASES + size, :] = jnp.dot(perm, rows, preferred_element_type=F32).astype(BF16)
        stores[c].start()
    for c in stores:
        c.wait()


def solution(mesh):
    head_groups = mesh.shape['tp']
    seq_size = mesh.shape['sp']

    def device_fn(hidden, w_query, w_key, w_value, w_out, branch_bias):
        tokens, model_width = hidden.shape
        num_branches, num_heads = branch_bias.shape
        dim = model_width // num_heads
        local_cols = w_query.shape[1]
        cols = model_width // head_groups
        half = tokens // PHASES // 2
        block_rows = min(256, tokens // 16)
        assert head_groups == 4 and num_branches == 4 and num_heads == PHASES and local_cols == 2 * dim
        assert half * PHASES == seg_rows(tokens) and local_cols == cols
        assert 3 * model_width >= 8 * 2 * half and model_width % (2 * half) == 0
        any_spec = pl.BlockSpec(memory_space=pl.ANY)
        dma = pltpu.SemaphoreType.DMA
        tile = (half, dim)
        vm = lambda *shape: pltpu.VMEM(shape, BF16)
        phase_major = pl.pallas_call(
            functools.partial(_layer, (block_rows, half, dim, dim ** -0.5)),
            out_shape=jax.ShapeDtypeStruct((PHASES, 2 * half, cols), BF16),
            in_specs=[any_spec] * 5 + [pl.BlockSpec(memory_space=pltpu.SMEM)],
            out_specs=any_spec,
            scratch_shapes=[
                vm(2, block_rows, model_width), vm(3, model_width, local_cols),
                pltpu.VMEM((6, dim // 128, block_rows, 128), F32),
                vm(2, PHASES, 2, *tile), vm(2, PHASES, 2, *tile), vm(2, PHASES, 2, *tile),
                vm(2, 2, 2, *tile), vm(2, 2, 2, *tile), vm(3, 2, 2, *tile), vm(3, 2, 2, *tile),
                vm(seq_size, head_groups, local_cols // seq_size, model_width),
                vm(10, 2, 2, 2, *tile),
                dma((2,)), dma((3,)), dma((seq_size,)),
                dma((2,)), dma((2,)), dma((2,)), dma((2,)), dma((2, 3)), dma((2, 3)), dma((2, 3)), dma((2, 3)),
                dma((3, 3)), dma((3, 3)), dma((2, 3)), dma((2, 3)),
                dma((2, 2)), dma((2, 2)), dma((3, 2, 2)), dma((3, 2, 2)),
                dma((4, 2)), dma((4, 2)), dma((2, 2)), dma((2, 2)), dma((4, 2, 2)), dma((4, 2, 2)), dma((2, 2, 2)),
                dma((2, 2, 2)), dma((2, 2)), dma((2, 2)), dma((2, 2)),
            ],
            compiler_params=pltpu.CompilerParams(collective_id=0, has_side_effects=True,
                                                 vmem_limit_bytes=67043328),
            name='layer',
        )(hidden, w_query, w_key, w_value, w_out, branch_bias)
        return pl.pallas_call(
            _natural_order,
            in_specs=[any_spec],
            out_specs=any_spec,
            out_shape=jax.ShapeDtypeStruct((tokens, cols), BF16),
            scratch_shapes=[vm(PHASES, 2 * half, cols), vm(tokens, cols), dma((8,)), dma((8,))],
            name='natural_order',
        )(phase_major)

    return jax.shard_map(device_fn, mesh=mesh, in_specs=(P(('dp', 'sp'), None), P(None, 'tp'), P(None, 'tp'), P(None, 'tp'), P('tp', None), P(None, None)), out_specs=P(('dp', 'sp'), 'tp'), check_vma=False)


def seg_rows(tokens):
    return SEG_BASE if tokens >= 2 * SEG_BASE else tokens // 2
```
